32 devices in a mesh: group: 1, seq: 16 (over z, y, x), batch: 1, head: 2 (over core).
Axes of the slice: x: 2, y: 2, z: 4, core: 2. Of those that a mesh axis runs over, the one named last changes fastest.
Arguments:
- queries: bfloat16 [2, 4, 128, 576], P(('group', 'batch'), None, ('seq', 'head')), may hold values from -40 to 40
- cache: bfloat16 [2, 32768, 576], P(('group', 'batch'), 'seq'), may hold values from -6 to 6
- lengths: int32 [2], P(('group', 'batch')), may hold values from 5 to 32768, as said below
Outputs:
- attended: bfloat16 [2, 4, 128, 512], P(('group', 'batch'), None, ('seq', 'head'))
The draws below stay inside these ranges and needn't reach their ends.
Inputs may be any that keep to these rules, and one draw needn't show every extreme that they name: `lengths`: at least one sequence has length exactly 32768.
All inputs are finite; a program needn't handle non-finite values.
Results may differ from the reference program's by a relative error of at most 0.0065.
Values may be sent and summed in bfloat16 or wider, within the bound.
A program may use at most 64 MiB of HBM per device.

```python
import jax
import jax.numpy as jnp
from jax import lax

H = 128
LAT = 512
ROPE = 64
NOPE = 128
DRAFT = 4
TOK_DEV = 2048
KDIM = 576
B = 2
CTX = 32768


def cache_base(key):
    first = jax.random.fold_in(key, 0)
    base = jnp.clip(jax.random.normal(first, (B, CTX, KDIM), jnp.float32), -6.0, 6.0)
    return base


def draw_cache(key, part):
    return cache_base(jax.random.fold_in(key, 11)).astype(jnp.bfloat16)


def draw_queries(key, part):
    first = jax.random.fold_in(jax.random.fold_in(key, 23), 0)
    values = 1.5 * jnp.clip(jax.random.normal(first, (B, DRAFT, H, KDIM), jnp.float32), -6.0, 6.0)
    return values.astype(jnp.bfloat16)


def draw_lengths(key, part):
    first, second, third, fourth = jax.random.split(jax.random.fold_in(key, 37), 4)
    spread = jax.random.randint(first, (B,), DRAFT + 1, CTX + 1)
    longer = jax.random.randint(second, (B,), CTX - TOK_DEV, CTX + 1)
    coin = jax.random.randint(third, (B,), 0, 2)
    chosen = jax.random.randint(fourth, (), 0, B)
    result = jnp.where(coin == 1, longer, spread)
    result = jnp.where(jnp.arange(B, dtype=jnp.int32) == chosen, CTX, result)
    return result.astype(jnp.int32)


def setup_inputs(seed: int = 0, part: int = 0) -> dict:
    streams_of = jax.random.split(jax.random.key(seed), 4)
    own_keys = jax.random.split(jax.random.fold_in(streams_of[3], part), 4)
    queries = draw_queries(jax.random.fold_in(jax.random.fold_in(streams_of[3], part), 71), part)
    cache = draw_cache(jax.random.fold_in(jax.random.fold_in(streams_of[3], part), 71), part)
    lengths = draw_lengths(jax.random.fold_in(jax.random.fold_in(streams_of[3], part), 71), part)
    return dict(queries=queries, cache=cache, lengths=lengths)


def attend_sequence(items):
    query_rows, keys, length = items
    scale = (NOPE + ROPE) ** -0.5
    scores = jnp.einsum("dhk,tk->dht", query_rows.astype(jnp.float32), keys.astype(jnp.float32)) * scale
    limit = length - DRAFT + jnp.arange(DRAFT, dtype=jnp.int32)
    visible = jnp.arange(CTX, dtype=jnp.int32)[None, None, :] <= limit[:, None, None]
    masked = jnp.where(visible, scores, jnp.float32(-1e30))
    peak = jnp.max(masked, axis=2)
    weights = jnp.where(visible, jnp.exp(masked - peak[:, :, None]), jnp.float32(0.0))
    total = jnp.sum(weights, axis=2)
    rounded = weights.astype(jnp.bfloat16).astype(jnp.float32)
    numerator = jnp.einsum("dht,tl->dhl", rounded, keys[:, :LAT].astype(jnp.float32))
    return (numerator / total[:, :, None]).astype(jnp.bfloat16)


def reference(queries, cache, lengths):
    return lax.map(attend_sequence, (queries, cache, lengths.astype(jnp.int32)))
```

```python
import functools
import math

import jax
import jax.numpy as jnp
from jax import lax
from jax.experimental import pallas as pl
from jax.experimental.pallas import tpu as pltpu
from jax.sharding import PartitionSpec as P

LAT = 512
ROPE = 64
NOPE = 128
STAT = 128
MESH = pl.DeviceIdType.MESH
F32 = jnp.float32
BF16 = jnp.bfloat16


def kernel(
    planes,
    columns,
    len_ref,
    q_ref,
    cache_ref,
    out_ref,
    kv,
    gathered,
    scores,
    probs,
    part_out,
    part_in,
    line_out,
    line_in,
    kv_sem,
    z_send,
    z_recv,
    p_send,
    p_recv,
    a_send,
    a_recv,
    b_send,
    b_recv,
):
    batch, draft, heads, _ = q_ref.shape
    tokens = cache_ref.shape[2]
    rows = draft * heads
    total_rows = planes * columns * rows
    me = lax.axis_index("seq")
    z = me // planes
    p = me % planes
    scale = (NOPE + ROPE) ** (-0.5) * math.log2(math.e)

    def to_plane(j):
        if planes == 4:
            return (p + 1 - 2 * (p % 2), (p + 2) % 4, 3 - p)[j - 1]
        return (p + j) % planes

    def to_line(k):
        return (z + k) % columns

    def from_line(k):
        return (z + columns - k) % columns

    def remote(src, dst, send, recv, seq):
        return pltpu.make_async_remote_copy(
            src_ref=src,
            dst_ref=dst,
            send_sem=send,
            recv_sem=recv,
            device_id={"seq": seq},
            device_id_type=MESH,
        )

    loads = [
        pltpu.make_async_copy(cache_ref.at[b], kv.at[b], kv_sem.at[b]) for b in range(batch)
    ]
    for load in loads:
        load.start()

    barrier = pltpu.get_barrier_semaphore()
    peers = [z * planes + to_plane(j) for j in range(1, planes)]
    peers += [to_line(k) * planes + p for k in range(1, columns)]
    for peer in peers:
        pl.semaphore_signal(barrier, inc=1, device_id={"seq": peer}, device_id_type=MESH)

    for b in range(batch):
        for d in range(draft):
            gathered[b, p, z, d * heads : (d + 1) * heads, :] = q_ref[b, d]
    pl.semaphore_wait(barrier, len(peers))

    def line_copy(b, k):
        block = gathered.at[b, p, z]
        return remote(block, block, z_send.at[b, k], z_recv.at[b, k], to_line(k) * planes + p)

    def plane_copy(b, k, j):
        block = gathered.at[b, p, from_line(k)]
        return remote(
            block, block, p_send.at[b, k, j], p_recv.at[b, k, j], z * planes + to_plane(j)
        )

    sent = []
    for b in range(batch):
        for k in range(1, columns):
            copy = line_copy(b, k)
            copy.start()
            sent.append(copy)
    for b in range(batch):
        for k in range(columns):
            if k:
                line_copy(b, k).wait_recv()
            for j in range(planes - 1, 0, -1):
                copy = plane_copy(b, k, j)
                copy.start()
                sent.append(copy)

    tile = min(512, tokens)
    row = lax.broadcasted_iota(jnp.int32, (total_rows, 1), 0)
    step = (row % rows) // heads - draft - me * tokens
    lane = lax.broadcasted_iota(jnp.int32, (total_rows, tile), 1)
    stat_lane = lax.broadcasted_iota(jnp.int32, (total_rows, STAT), 1)

    def attend(b):
        q = gathered[b].reshape(total_rows, q_ref.shape[3])
        limit = step + len_ref[b]
        peak = jnp.full((total_rows, 1), -1e20, F32)
        for t in range(0, tokens, tile):
            s = lax.dot_general(
                q, kv[b, :, t : t + tile], (((1,), (0,)), ((), ())), preferred_element_type=F32
            )
            s = jnp.where(lane <= limit - t, s * scale, -1e30)
            scores[:, t : t + tile] = s
            peak = jnp.maximum(peak, jnp.max(s, axis=1, keepdims=True))
        peak = peak.astype(BF16).astype(F32)
        total = jnp.zeros((total_rows, 1), F32)
        for t in range(0, tokens, tile):
            w = jnp.exp2(scores[:, t : t + tile] - peak)
            total = total + jnp.sum(w, axis=1, keepdims=True)
            probs[:, t : t + tile] = w.astype(BF16)
        numerator = lax.dot_general(
            probs[...], kv[b, :LAT, :], (((1,), (1,)), ((), ())), preferred_element_type=F32
        )
        part_out[b, :, :, :, :LAT] = numerator.astype(BF16).reshape(planes, columns, rows, LAT)
        part_out[b, :, :, :, LAT:] = pack(stat_lane, peak, total).reshape(
            planes, columns, rows, STAT
        )

    def pack(lanes, peak, total):
        high = total.astype(BF16).astype(F32)
        stats = jnp.where(lanes == 0, peak, jnp.where(lanes == 1, high, total - high))
        return stats.astype(BF16)

    def merge(parts):
        stats = [x[:, LAT:].astype(F32) for x in parts]
        peaks = [x[:, 0:1] for x in stats]
        peak = functools.reduce(jnp.maximum, peaks)
        factors = [jnp.exp2(x - peak) for x in peaks]
        total = sum(f * (x[:, 1:2] + x[:, 2:3]) for f, x in zip(factors, stats))
        numerator = sum(f * x[:, :LAT].astype(F32) for f, x in zip(factors, parts))
        return numerator, peak, total

    def plane_part(b, j):
        other = to_plane(j)
        return remote(
            part_out.at[b, other],
            part_in.at[b, j],
            a_send.at[b, j],
            a_recv.at[b, j],
            z * planes + other,
        )

    def line_part(b, k):
        other = to_line(k)
        return remote(
            line_out.at[b, other],
            line_in.at[b, k],
            b_send.at[b, k],
            b_recv.at[b, k],
            other * planes + p,
        )

    for b in range(batch):
        for k in range(columns):
            for j in range(planes - 1, 0, -1):
                plane_copy(b, k, j).wait_recv()
        loads[b].wait()
        attend(b)
        for j in range(planes - 1, 0, -1):
            copy = plane_part(b, j)
            copy.start()
            sent.append(copy)

    line_rows = columns * rows
    for b in range(batch):
        parts = [part_out[b, p].reshape(line_rows, LAT + STAT)]
        for j in range(1, planes):
            plane_part(b, j).wait_recv()
            parts.append(part_in[b, j].reshape(line_rows, LAT + STAT))
        numerator, peak, total = merge(parts)
        line_out[b, :, :, :LAT] = numerator.astype(BF16).reshape(columns, rows, LAT)
        line_out[b, :, :, LAT:] = pack(stat_lane[:line_rows], peak, total).reshape(
            columns, rows, STAT
        )
        for k in range(columns - 1, 0, -1):
            copy = line_part(b, k)
            copy.start()
            sent.append(copy)

    for b in range(batch):
        parts = [line_out[b, z]]
        for k in range(1, columns):
            line_part(b, k).wait_recv()
            parts.append(line_in[b, k])
        numerator, peak, total = merge(parts)
        result = (numerator / total).astype(BF16)
        for d in range(draft):
            out_ref[b, d] = result[d * heads : (d + 1) * heads]

    for copy in sent:
        copy.wait_send()


def body(ways, queries, cache, lengths):
    batch, draft, heads, depth = queries.shape
    tokens = cache.shape[1]
    rows = draft * heads
    planes = max(i for i in range(1, ways + 1) if ways % i == 0 and i * i <= ways)
    columns = ways // planes
    vmem = pl.BlockSpec(memory_space=pltpu.VMEM)
    dma = pltpu.SemaphoreType.DMA
    width = LAT + STAT
    return pl.pallas_call(
        functools.partial(kernel, planes, columns),
        out_shape=jax.ShapeDtypeStruct((batch, draft, heads, LAT), BF16),
        in_specs=[
            pl.BlockSpec(memory_space=pltpu.SMEM),
            vmem,
            pl.BlockSpec(memory_space=pltpu.HBM),
        ],
        out_specs=vmem,
        scratch_shapes=[
            pltpu.VMEM((batch, depth, tokens), BF16),
            pltpu.VMEM((batch, planes, columns, rows, depth), BF16),
            pltpu.VMEM((ways * rows, tokens), F32),
            pltpu.VMEM((ways * rows, tokens), BF16),
            pltpu.VMEM((batch, planes, columns, rows, width), BF16),
            pltpu.VMEM((batch, planes, columns, rows, width), BF16),
            pltpu.VMEM((batch, columns, rows, width), BF16),
            pltpu.VMEM((batch, columns, rows, width), BF16),
            dma((batch,)),
            dma((batch, columns)),
            dma((batch, columns)),
            dma((batch, columns, planes)),
            dma((batch, columns, planes)),
            dma((batch, planes)),
            dma((batch, planes)),
            dma((batch, columns)),
            dma((batch, columns)),
        ],
        compiler_params=pltpu.CompilerParams(
            collective_id=0,
            has_side_effects=True,
            vmem_limit_bytes=48 * 1024 * 1024,
        ),
    )(lengths, queries, jnp.swapaxes(cache, 1, 2))


def solution(mesh):
    return jax.shard_map(
        functools.partial(body, mesh.shape["seq"]),
        mesh=mesh,
        in_specs=(
            P(("group", "batch"), None, ("seq", "head"), None),
            P(("group", "batch"), "seq", None),
            P(("group", "batch")),
        ),
        out_specs=P(("group", "batch"), None, ("seq", "head"), None),
        check_vma=False,
    )
```

```python
import functools
import math

import jax
import jax.numpy as jnp
from jax import lax
from jax.experimental import pallas as pl
from jax.experimental.pallas import tpu as pltpu
from jax.sharding import PartitionSpec as P

LAT = 512
ROPE = 64
NOPE = 128
STAT = 128
MESH = pl.DeviceIdType.MESH
F32 = jnp.float32
BF16 = jnp.bfloat16


def kernel(
    planes,
    columns,
    len_hbm,
    q_hbm,
    cache_ref,
    out_ref,
    len_ref,
    q_ref,
    kv,
    gathered,
    scores,
    probs,
    part_out,
    part_in,
    stat_out,
    stat_in,
    line_out,
    line_in,
    in_sem,
    kv_sem,
    z_send,
    z_recv,
    p_send,
    p_recv,
    a_send,
    a_recv,
    s_send,
    s_recv,
    b_send,
    b_recv,
):
    batch, draft, heads, _ = q_ref.shape
    tokens = cache_ref.shape[2]
    rows = draft * heads
    total_rows = planes * columns * rows
    me = lax.axis_index("seq")
    z = me // planes
    p = me % planes
    scale = (NOPE + ROPE) ** (-0.5) * math.log2(math.e)

    def to_plane(j):
        if planes == 4:
            return (p + 1 - 2 * (p % 2), (p + 2) % 4, 3 - p)[j - 1]
        return (p + j) % planes

    half = z // (columns - columns // 2)
    far = (1 - half) * (columns - 1)
    gap = far + (2 * half - 1) * z

    def line(i):
        return far + (2 * half - 1) * (i + (i + columns - gap) // columns)

    def remote(src, dst, send, recv, seq):
        return pltpu.make_async_remote_copy(
            src_ref=src,
            dst_ref=dst,
            send_sem=send,
            recv_sem=recv,
            device_id={"seq": seq},
            device_id_type=MESH,
        )

    loads = [
        pltpu.make_async_copy(cache_ref.at[b], kv.at[b], kv_sem.at[b]) for b in range(batch)
    ]
    small = [
        pltpu.make_async_copy(q_hbm, q_ref, in_sem.at[0]),
        pltpu.make_async_copy(len_hbm, len_ref, in_sem.at[1]),
    ]
    for load in small:
        load.start()

    barrier = pltpu.get_barrier_semaphore()
    peers = [z * planes + to_plane(j) for j in range(1, planes)]
    peers += [line(i) * planes + p for i in range(columns - 1)]
    for peer in peers:
        pl.semaphore_signal(barrier, inc=1, device_id={"seq": peer}, device_id_type=MESH)

    for load in loads:
        load.start()
    for load in small:
        load.wait()
    for b in range(batch):
        for d in range(draft):
            gathered[b, p, z, d * heads : (d + 1) * heads, :] = q_ref[b, d]
    pl.semaphore_wait(barrier, len(peers))

    def line_copy(b, i):
        block = gathered.at[b, p, z]
        return remote(block, block, z_send.at[b, i], z_recv.at[b, z], line(i) * planes + p)

    def line_arrival(b, i):
        other = line(i)
        block = gathered.at[b, p, other]
        return remote(block, block, z_send.at[b, i], z_recv.at[b, other], other * planes + p)

    def plane_copy(b, source, j):
        block = gathered.at[b, p, source]
        return remote(
            block,
            block,
            p_send.at[b, source, j],
            p_recv.at[b, source, j],
            z * planes + to_plane(j),
        )

    sent = []

    def start(copy):
        copy.start()
        sent.append(copy)

    for b in range(batch):
        for i in range(columns - 1):
            start(line_copy(b, i))
    for b in range(batch):
        for j in range(planes - 1, 0, -1):
            start(plane_copy(b, z, j))
    for b in range(batch):
        for i in range(columns - 2, -1, -1):
            line_arrival(b, i).wait_recv()
            for j in range(planes - 1, 0, -1):
                start(plane_copy(b, line(i), j))

    tile = min(512, tokens)
    row = lax.broadcasted_iota(jnp.int32, (total_rows, 1), 0)
    step = (row % rows) // heads - draft - me * tokens
    lane = lax.broadcasted_iota(jnp.int32, (total_rows, tile), 1)
    stat_lane = lax.broadcasted_iota(jnp.int32, (planes, rows, STAT), 2)

    def attend(b):
        q = gathered[b].reshape(total_rows, q_ref.shape[3])
        limit = step + len_ref[b]
        peak = jnp.full((total_rows, 1), -1e20, F32)
        for t in range(0, tokens, tile):
            s = lax.dot_general(
                q, kv[b, :, t : t + tile], (((1,), (0,)), ((), ())), preferred_element_type=F32
            )
            s = jnp.where(lane <= limit - t, s * scale, -1e30)
            scores[:, t : t + tile] = s
            peak = jnp.maximum(peak, jnp.max(s, axis=1, keepdims=True))
        peak = peak.astype(BF16).astype(F32)
        total = jnp.zeros((total_rows, 1), F32)
        for t in range(0, tokens, tile):
            w = jnp.exp2(scores[:, t : t + tile] - peak)
            total = total + jnp.sum(w, axis=1, keepdims=True)
            probs[:, t : t + tile] = w.astype(BF16)
        numerator = lax.dot_general(
            probs[...], kv[b, :LAT, :], (((1,), (1,)), ((), ())), preferred_element_type=F32
        )
        part_out[b] = numerator.astype(BF16).reshape(planes, columns, rows, LAT)
        high = total.astype(BF16).astype(F32)
        stats = jnp.zeros((planes, rows, STAT), F32)
        for n, x in enumerate((peak, high, total - high)):
            x = x.reshape(planes, columns, rows, 1)
            for c in range(columns):
                stats = jnp.where(stat_lane == 3 * c + n, x[:, c], stats)
        stat_out[b] = stats.astype(BF16)

    def merge(stats, parts):
        peak = functools.reduce(jnp.maximum, [x[0] for x in stats])
        factors = [jnp.exp2(x[0] - peak) for x in stats]
        total = sum(f * (x[1] + x[2]) for f, x in zip(factors, stats))
        numerator = sum(f * x.astype(F32) for f, x in zip(factors, parts))
        return numerator, peak, total

    small_lane = lax.broadcasted_iota(jnp.int32, (rows, STAT), 1)

    def plane_stats(x, c):
        x = x.astype(F32)
        return [
            jnp.sum(jnp.where(small_lane == 3 * c + n, x, 0.0), axis=1, keepdims=True)
            for n in range(3)
        ]

    def line_stats(tile):
        x = tile[:, LAT:].astype(F32)
        return [x[:, n : n + 1] for n in range(3)]

    def plane_part(b, c, j):
        other = to_plane(j)
        return remote(
            part_out.at[b, other, c],
            part_in.at[b, j, c],
            a_send.at[b, c, j],
            a_recv.at[b, c, j],
            z * planes + other,
        )

    def plane_stat(b, j):
        other = to_plane(j)
        return remote(
            stat_out.at[b, other],
            stat_in.at[b, j],
            s_send.at[b, j],
            s_recv.at[b, j],
            z * planes + other,
        )

    def line_part(b, i):
        other = line(i)
        return remote(
            line_out.at[b, other],
            line_in.at[b, z],
            b_send.at[b, i],
            b_recv.at[b, z],
            other * planes + p,
        )

    def line_part_arrival(b, i):
        other = line(i)
        return remote(
            line_out.at[b, other],
            line_in.at[b, other],
            b_send.at[b, i],
            b_recv.at[b, other],
            other * planes + p,
        )

    def plane_merge(b, c):
        parts = [part_out[b, p, c]]
        stats = [plane_stats(stat_out[b, p], c)]
        for j in range(1, planes):
            plane_part(b, c, j).wait_recv()
            parts.append(part_in[b, j, c])
            stats.append(plane_stats(stat_in[b, j], c))
        return merge(stats, parts)

    order = [line(i) for i in range(columns - 1)] + [z]
    for b in range(batch):
        for c in range(columns):
            for j in range(planes - 1, 0, -1):
                plane_copy(b, c, j).wait_recv()
        loads[b].wait()
        attend(b)
        for j in range(planes - 1, 0, -1):
            start(plane_stat(b, j))
        for c in order:
            for j in range(planes - 1, 0, -1):
                start(plane_part(b, c, j))

    own = []
    for b in range(batch):
        for j in range(1, planes):
            plane_stat(b, j).wait_recv()
        for i in range(columns - 1):
            numerator, peak, total = plane_merge(b, line(i))
            high = total.astype(BF16).astype(F32)
            packed = jnp.where(
                small_lane == 0, peak, jnp.where(small_lane == 1, high, total - high)
            )
            line_out[b, line(i), :, :LAT] = numerator.astype(BF16)
            line_out[b, line(i), :, LAT:] = packed.astype(BF16)
            start(line_part(b, i))
        own.append(plane_merge(b, z))

    for b in range(batch):
        numerator, peak, total = own[b]
        stats, parts = [[peak, total, 0.0]], [numerator]
        for i in range(columns - 2, -1, -1):
            line_part_arrival(b, i).wait_recv()
            block = line_in[b, line(i)]
            stats.append(line_stats(block))
            parts.append(block[:, :LAT])
        numerator, _, total = merge(stats, parts)
        result = (numerator / total).astype(BF16)
        for d in range(draft):
            out_ref[b, d] = result[d * heads : (d + 1) * heads]

    for copy in sent:
        copy.wait_send()


def body(ways, queries, cache, lengths):
    batch, draft, heads, depth = queries.shape
    tokens = cache.shape[1]
    rows = draft * heads
    planes = max(i for i in range(1, ways + 1) if ways % i == 0 and i * i <= ways)
    columns = ways // planes
    dma = pltpu.SemaphoreType.DMA
    width = LAT + STAT
    return pl.pallas_call(
        functools.partial(kernel, planes, columns),
        out_shape=jax.ShapeDtypeStruct((batch, draft, heads, LAT), BF16),
        in_specs=[
            pl.BlockSpec(memory_space=pl.ANY),
            pl.BlockSpec(memory_space=pl.ANY),
            pl.BlockSpec(memory_space=pl.ANY),
        ],
        out_specs=pl.BlockSpec(memory_space=pltpu.VMEM),
        scratch_shapes=[
            pltpu.SMEM(lengths.shape, jnp.int32),
            pltpu.VMEM(queries.shape, BF16),
            pltpu.VMEM((batch, depth, tokens), BF16),
            pltpu.VMEM((batch, planes, columns, rows, depth), BF16),
            pltpu.VMEM((ways * rows, tokens), F32),
            pltpu.VMEM((ways * rows, tokens), BF16),
            pltpu.VMEM((batch, planes, columns, rows, LAT), BF16),
            pltpu.VMEM((batch, planes, columns, rows, LAT), BF16),
            pltpu.VMEM((batch, planes, rows, STAT), BF16),
            pltpu.VMEM((batch, planes, rows, STAT), BF16),
            pltpu.VMEM((batch, columns, rows, width), BF16),
            pltpu.VMEM((batch, columns, rows, width), BF16),
            dma((2,)),
            dma((batch,)),
            dma((batch, columns)),
            dma((batch, columns)),
            dma((batch, columns, planes)),
            dma((batch, columns, planes)),
            dma((batch, columns, planes)),
            dma((batch, columns, planes)),
            dma((batch, planes)),
            dma((batch, planes)),
            dma((batch, columns)),
            dma((batch, columns)),
        ],
        compiler_params=pltpu.CompilerParams(
            collective_id=0,
            has_side_effects=True,
            vmem_limit_bytes=50331648,
        ),
    )(pltpu.with_memory_space_constraint(lengths, pltpu.HBM), pltpu.with_memory_space_constraint(queries, pltpu.HBM), pltpu.with_memory_space_constraint(jnp.swapaxes(cache, 1, 2), pltpu.HBM))


def solution(mesh):
    return jax.shard_map(
        functools.partial(body, mesh.shape["seq"]),
        mesh=mesh,
        in_specs=(
            P(("group", "batch"), None, ("seq", "head"), None),
            P(("group", "batch"), "seq", None),
            P(("group", "batch")),
        ),
        out_specs=P(("group", "batch"), None, ("seq", "head"), None),
        check_vma=False,
    )
```

```python
import functools
import math

import jax
import jax.numpy as jnp
from jax import lax
from jax.experimental import pallas as pl
from jax.experimental.pallas import tpu as pltpu
from jax.sharding import PartitionSpec as P

LAT = 512
ROPE = 64
NOPE = 128
STAT = 128
MESH = pl.DeviceIdType.MESH
F32 = jnp.float32
BF16 = jnp.bfloat16


def kernel(
    planes,
    columns,
    len_hbm,
    q_hbm,
    cache_ref,
    out_ref,
    len_ref,
    q_ref,
    kv,
    gathered,
    scores,
    probs,
    part_out,
    part_in,
    stat_out,
    stat_in,
    line_out,
    line_in,
    in_sem,
    kv_sem,
    z_send,
    z_recv,
    p_send,
    p_recv,
    a_send,
    a_recv,
    s_send,
    s_recv,
    b_send,
    b_recv,
):
    batch, draft, heads, _ = q_ref.shape
    tokens = cache_ref.shape[2]
    rows = draft * heads
    total_rows = planes * columns * rows
    me = lax.axis_index("seq")
    z = me // planes
    p = me % planes
    scale = (NOPE + ROPE) ** (-0.5) * math.log2(math.e)

    def to_plane(j):
        if planes == 4:
            return (p + 1 - 2 * (p % 2), (p + 2) % 4, 3 - p)[j - 1]
        return (p + j) % planes

    half = z // (columns - columns // 2)
    far = (1 - half) * (columns - 1)
    gap = far + (2 * half - 1) * z

    def line(i):
        return far + (2 * half - 1) * (i + (i + columns - gap) // columns)

    def remote(src, dst, send, recv, seq):
        return pltpu.make_async_remote_copy(
            src_ref=src,
            dst_ref=dst,
            send_sem=send,
            recv_sem=recv,
            device_id={"seq": seq},
            device_id_type=MESH,
        )

    loads = [
        pltpu.make_async_copy(cache_ref.at[b], kv.at[b], kv_sem.at[b]) for b in range(batch)
    ]
    small = [
        pltpu.make_async_copy(q_hbm, q_ref, in_sem.at[0]),
        pltpu.make_async_copy(len_hbm, len_ref, in_sem.at[1]),
    ]
    for load in small:
        load.start()

    barrier = pltpu.get_barrier_semaphore()
    peers = [z * planes + to_plane(j) for j in range(1, planes)]
    peers += [line(i) * planes + p for i in range(columns - 1)]
    for peer in peers:
        pl.semaphore_signal(barrier, inc=1, device_id={"seq": peer}, device_id_type=MESH)

    for load in loads:
        load.start()
    for load in small:
        load.wait()
    for b in range(batch):
        for d in range(draft):
            gathered[b, p, z, d * heads : (d + 1) * heads, :] = q_ref[b, d]
    pl.semaphore_wait(barrier, len(peers))

    def line_copy(b, i):
        block = gathered.at[b, p, z]
        return remote(block, block, z_send.at[b, i], z_recv.at[b, z], line(i) * planes + p)

    def line_arrival(b, i):
        other = line(i)
        block = gathered.at[b, p, other]
        return remote(block, block, z_send.at[b, i], z_recv.at[b, other], other * planes + p)

    def plane_copy(b, source, j):
        block = gathered.at[b, p, source]
        return remote(
            block,
            block,
            p_send.at[b, source, j],
            p_recv.at[b, source, j],
            z * planes + to_plane(j),
        )

    sent = []

    def start(copy):
        copy.start()
        sent.append(copy)

    for b in range(batch):
        for i in range(columns - 1):
            start(line_copy(b, i))
    for b in range(batch):
        for j in range(planes - 1, 0, -1):
            start(plane_copy(b, z, j))
    for b in range(batch):
        for i in range(columns - 2, -1, -1):
            line_arrival(b, i).wait_recv()
            for j in range(planes - 1, 0, -1):
                start(plane_copy(b, line(i), j))

    tile = min(256, tokens)
    row = lax.broadcasted_iota(jnp.int32, (total_rows, 1), 0)
    step = (row % rows) // heads - draft - me * tokens
    lane = lax.broadcasted_iota(jnp.int32, (total_rows, tile), 1)
    stat_lane = lax.broadcasted_iota(jnp.int32, (planes, rows, STAT), 2)

    def attend(b):
        q = gathered[b].reshape(total_rows, q_ref.shape[3])
        limit = step + len_ref[b]
        peak = jnp.full((total_rows, 1), -1e20, F32)
        for t in range(0, tokens, tile):
            s = lax.dot_general(
                q, kv[b, :, t : t + tile], (((1,), (0,)), ((), ())), preferred_element_type=F32
            )
            s = jnp.where(lane <= limit - t, s * scale, -1e30)
            scores[:, t : t + tile] = s
            peak = jnp.maximum(peak, jnp.max(s, axis=1, keepdims=True))
        peak = peak.astype(BF16).astype(F32)
        total = jnp.zeros((total_rows, 1), F32)
        for t in range(0, tokens, tile):
            w = jnp.exp2(scores[:, t : t + tile] - peak)
            total = total + jnp.sum(w, axis=1, keepdims=True)
            probs[:, t : t + tile] = w.astype(BF16)
        numerator = lax.dot_general(
            probs[...], kv[b, :LAT, :], (((1,), (1,)), ((), ())), preferred_element_type=F32
        )
        part_out[b] = numerator.astype(BF16).reshape(planes, columns, rows, LAT)
        high = total.astype(BF16).astype(F32)
        stats = jnp.zeros((planes, rows, STAT), F32)
        for n, x in enumerate((peak, high, total - high)):
            x = x.reshape(planes, columns, rows, 1)
            for c in range(columns):
                stats = jnp.where(stat_lane == 3 * c + n, x[:, c], stats)
        stat_out[b] = stats.astype(BF16)

    def merge(stats, parts):
        peak = functools.reduce(jnp.maximum, [x[0] for x in stats])
        factors = [jnp.exp2(x[0] - peak) for x in stats]
        total = sum(f * (x[1] + x[2]) for f, x in zip(factors, stats))
        numerator = sum(f * x.astype(F32) for f, x in zip(factors, parts))
        return numerator, peak, total

    small_lane = lax.broadcasted_iota(jnp.int32, (rows, STAT), 1)

    def plane_stats(x, c):
        x = x.astype(F32)
        return [
            jnp.sum(jnp.where(small_lane == 3 * c + n, x, 0.0), axis=1, keepdims=True)
            for n in range(3)
        ]

    def line_stats(tile):
        x = tile[:, LAT:].astype(F32)
        return [x[:, n : n + 1] for n in range(3)]

    def plane_part(b, c, j):
        other = to_plane(j)
        return remote(
            part_out.at[b, other, c],
            part_in.at[b, j, c],
            a_send.at[b, c, j],
            a_recv.at[b, c, j],
            z * planes + other,
        )

    def plane_stat(b, j):
        other = to_plane(j)
        return remote(
            stat_out.at[b, other],
            stat_in.at[b, j],
            s_send.at[b, j],
            s_recv.at[b, j],
            z * planes + other,
        )

    def line_part(b, i):
        other = line(i)
        return remote(
            line_out.at[b, other],
            line_in.at[b, z],
            b_send.at[b, i],
            b_recv.at[b, z],
            other * planes + p,
        )

    def line_part_arrival(b, i):
        other = line(i)
        return remote(
            line_out.at[b, other],
            line_in.at[b, other],
            b_send.at[b, i],
            b_recv.at[b, other],
            other * planes + p,
        )

    def plane_merge(b, c):
        parts = [part_out[b, p, c]]
        stats = [plane_stats(stat_out[b, p], c)]
        for j in range(1, planes):
            plane_part(b, c, j).wait_recv()
            parts.append(part_in[b, j, c])
            stats.append(plane_stats(stat_in[b, j], c))
        return merge(stats, parts)

    order = [line(i) for i in range(columns - 1)] + [z]
    for b in range(batch):
        for c in range(columns):
            for j in range(planes - 1, 0, -1):
                plane_copy(b, c, j).wait_recv()
        loads[b].wait()
        attend(b)
        for j in range(planes - 1, 0, -1):
            start(plane_stat(b, j))
        for c in order:
            for j in range(planes - 1, 0, -1):
                start(plane_part(b, c, j))

    own = []
    for b in range(batch):
        for j in range(1, planes):
            plane_stat(b, j).wait_recv()
        for i in range(columns - 1):
            numerator, peak, total = plane_merge(b, line(i))
            high = total.astype(BF16).astype(F32)
            packed = jnp.where(
                small_lane == 0, peak, jnp.where(small_lane == 1, high, total - high)
            )
            line_out[b, line(i), :, :LAT] = numerator.astype(BF16)
            line_out[b, line(i), :, LAT:] = packed.astype(BF16)
            start(line_part(b, i))
        own.append(plane_merge(b, z))

    for b in range(batch):
        numerator, peak, total = own[b]
        stats, parts = [[peak, total, 0.0]], [numerator]
        for i in range(columns - 2, -1, -1):
            line_part_arrival(b, i).wait_recv()
            block = line_in[b, line(i)]
            stats.append(line_stats(block))
            parts.append(block[:, :LAT])
        numerator, _, total = merge(stats, parts)
        result = (numerator / total).astype(BF16)
        for d in range(draft):
            out_ref[b, d] = result[d * heads : (d + 1) * heads]

    for copy in sent:
        copy.wait_send()


def body(ways, queries, cache, lengths):
    batch, draft, heads, depth = queries.shape
    tokens = cache.shape[1]
    rows = draft * heads
    planes = max(i for i in range(1, ways + 1) if ways % i == 0 and i * i <= ways)
    columns = ways // planes
    dma = pltpu.SemaphoreType.DMA
    width = LAT + STAT
    return pl.pallas_call(
        functools.partial(kernel, planes, columns),
        out_shape=jax.ShapeDtypeStruct((batch, draft, heads, LAT), BF16),
        in_specs=[
            pl.BlockSpec(memory_space=pl.ANY),
            pl.BlockSpec(memory_space=pl.ANY),
            pl.BlockSpec(memory_space=pl.ANY),
        ],
        out_specs=pl.BlockSpec(memory_space=pltpu.VMEM),
        scratch_shapes=[
            pltpu.SMEM(lengths.shape, jnp.int32),
            pltpu.VMEM(queries.shape, BF16),
            pltpu.VMEM((batch, depth, tokens), BF16),
            pltpu.VMEM((batch, planes, columns, rows, depth), BF16),
            pltpu.VMEM((ways * rows, tokens), F32),
            pltpu.VMEM((ways * rows, tokens), BF16),
            pltpu.VMEM((batch, planes, columns, rows, LAT), BF16),
            pltpu.VMEM((batch, planes, columns, rows, LAT), BF16),
            pltpu.VMEM((batch, planes, rows, STAT), BF16),
            pltpu.VMEM((batch, planes, rows, STAT), BF16),
            pltpu.VMEM((batch, columns, rows, width), BF16),
            pltpu.VMEM((batch, columns, rows, width), BF16),
            dma((2,)),
            dma((batch,)),
            dma((batch, columns)),
            dma((batch, columns)),
            dma((batch, columns, planes)),
            dma((batch, columns, planes)),
            dma((batch, columns, planes)),
            dma((batch, columns, planes)),
            dma((batch, planes)),
            dma((batch, planes)),
            dma((batch, columns)),
            dma((batch, columns)),
        ],
        compiler_params=pltpu.CompilerParams(
            collective_id=0,
            has_side_effects=True,
            vmem_limit_bytes=50331648,
        ),
    )(pltpu.with_memory_space_constraint(lengths, pltpu.HBM), pltpu.with_memory_space_constraint(queries, pltpu.HBM), pltpu.with_memory_space_constraint(jnp.swapaxes(cache, 1, 2), pltpu.HBM))


def solution(mesh):
    return jax.shard_map(
        functools.partial(body, mesh.shape["seq"]),
        mesh=mesh,
        in_specs=(
            P(("group", "batch"), None, ("seq", "head"), None),
            P(("group", "batch"), "seq", None),
            P(("group", "batch")),
        ),
        out_specs=P(("group", "batch"), None, ("seq", "head"), None),
        check_vma=False,
    )
```
